16 devices in a mesh: dp: 4 (over z, y), tp: 4 (over x, core).
Axes of the slice: x: 2, y: 2, z: 2, core: 2. Of those that a mesh axis runs over, the one named last changes fastest.
Arguments:
- hidden: bfloat16 [512, 4096], P('dp'), parts along dimension 0
- positions: int32 [512], P('dp'), parts along dimension 0
- k_cache: bfloat16 [2, 512, 64, 8, 128], P(None, 'dp', None, 'tp'), parts along dimension 1
- v_cache: bfloat16 [2, 512, 64, 8, 128], P(None, 'dp', None, 'tp'), parts along dimension 1
- attn_norm: bfloat16 [2, 4096], replicated
- w_query: bfloat16 [2, 4096, 4096], P(None, None, 'tp')
- w_key: bfloat16 [2, 4096, 1024], P(None, None, 'tp')
- w_value: bfloat16 [2, 4096, 1024], P(None, None, 'tp')
- w_out: bfloat16 [2, 4096, 4096], P(None, 'tp')
- mlp_norm: bfloat16 [2, 4096], replicated
- w_gate: bfloat16 [2, 4096, 14336], P(None, None, 'tp')
- w_up: bfloat16 [2, 4096, 14336], P(None, None, 'tp')
- w_down: bfloat16 [2, 14336, 4096], P(None, 'tp')
Outputs:
- output 1: bfloat16 [512, 4096], P('dp'), parts along dimension 0
- output 2: bfloat16 [2, 512, 64, 8, 128], P(None, 'dp', None, 'tp'), parts along dimension 1
- output 3: bfloat16 [2, 512, 64, 8, 128], P(None, 'dp', None, 'tp'), parts along dimension 1
There are 4 independent parts. The reference program is written for one: setup_inputs(seed, part) draws one part's arguments, and reference() takes and returns one part's arrays. A program takes and returns all parts, laid end to end along the dimension named above; an argument that names none is the same for every part.
All inputs are finite; a program needn't handle non-finite values.
Results may differ from the reference program's by a relative error of at most 0.02.
Values are sent between devices in bfloat16 or wider.
A program may use at most 1 GiB of HBM per device.

```python
import math
import jax
import jax.numpy as jnp
from jax import lax

LAYERS = 2
BATCH = 128
SEQ = 64
D = 4096
HEADS = 32
KV_HEADS = 8
HEAD = 128
FF = 14336


def normal_weight(rng_key, shape, scale):
    return (jax.random.normal(rng_key, shape, jnp.float32) * scale).astype(jnp.bfloat16)


def setup_inputs(seed: int = 0, part: int = 0) -> dict:
    base_key = jax.random.key(seed)
    shared_keys = jax.random.split(base_key, 9)
    part_keys = jax.random.split(jax.random.fold_in(base_key, part), 5)
    cache_shape = (LAYERS, BATCH, SEQ, KV_HEADS, HEAD)
    drawn_pos = jax.random.randint(part_keys[1], (BATCH,), SEQ // 8, SEQ, dtype=jnp.int32)
    drawn_pos = drawn_pos.at[0].set(SEQ - 1).at[1].set(SEQ // 8)
    return dict(
        hidden=normal_weight(part_keys[0], (BATCH, D), 1.0),
        positions=jax.random.permutation(part_keys[2], drawn_pos),
        k_cache=normal_weight(part_keys[3], cache_shape, 1.0),
        v_cache=normal_weight(part_keys[4], cache_shape, 1.0),
        attn_norm=(1.0 + 0.3 * jax.random.normal(shared_keys[0], (LAYERS, D), jnp.float32)).astype(jnp.bfloat16),
        w_query=normal_weight(shared_keys[1], (LAYERS, D, HEADS * HEAD), D ** -0.5),
        w_key=normal_weight(shared_keys[2], (LAYERS, D, KV_HEADS * HEAD), 1.5 * D ** -0.5),
        w_value=normal_weight(shared_keys[3], (LAYERS, D, KV_HEADS * HEAD), 1.5 * D ** -0.5),
        w_out=normal_weight(shared_keys[4], (LAYERS, HEADS * HEAD, D), 0.5 * (SEQ / (HEADS * HEAD)) ** 0.5),
        mlp_norm=(1.0 + 0.3 * jax.random.normal(shared_keys[5], (LAYERS, D), jnp.float32)).astype(jnp.bfloat16),
        w_gate=normal_weight(shared_keys[6], (LAYERS, D, FF), D ** -0.5),
        w_up=normal_weight(shared_keys[7], (LAYERS, D, FF), D ** -0.5),
        w_down=normal_weight(shared_keys[8], (LAYERS, FF, D), 1.5 * FF ** -0.5),
    )


def rms_norm(hidden, weight):
    hidden_f32 = hidden.astype(jnp.float32)
    mean_sq = jnp.mean(hidden_f32 * hidden_f32, axis=-1, keepdims=True)
    return (hidden_f32 * lax.rsqrt(mean_sq + 1e-5) * weight.astype(jnp.float32)).astype(jnp.bfloat16)


def rope_tables(positions, head_dim):
    half_dim = head_dim // 2
    inv_freq = jnp.power(500000.0, -jnp.arange(half_dim, dtype=jnp.float32) * (2.0 / head_dim))
    wavelen = (2.0 * math.pi) / inv_freq
    smooth = (8192.0 / wavelen - 1.0) / 3.0
    blended = (1.0 - smooth) * inv_freq / 8.0 + smooth * inv_freq
    scaled = jnp.where(wavelen < 2048.0, inv_freq, jnp.where(wavelen > 8192.0, inv_freq / 8.0, blended))
    angles = positions.astype(jnp.float32)[:, None] * scaled[None, :]
    return jnp.cos(angles), jnp.sin(angles)


def apply_rope(vectors, cos_tab, sin_tab):
    half_dim = vectors.shape[-1] // 2
    vec_f32 = vectors.astype(jnp.float32)
    first = vec_f32[..., :half_dim]
    second = vec_f32[..., half_dim:]
    cos_b = cos_tab[:, None, :]
    sin_b = sin_tab[:, None, :]
    return jnp.concatenate([first * cos_b - second * sin_b, second * cos_b + first * sin_b], axis=-1).astype(jnp.bfloat16)


def attend(query, k_all, v_all, visible):
    scores = jnp.einsum('bkgd,bskd->bkgs', query.astype(jnp.float32), k_all.astype(jnp.float32)) * (query.shape[-1] ** -0.5)
    scores = jnp.where(visible, scores, -jnp.inf)
    prob_rows = jax.nn.softmax(scores, axis=-1).astype(jnp.bfloat16)
    attn_out = jnp.einsum('bkgs,bskd->bkgd', prob_rows.astype(jnp.float32), v_all.astype(jnp.float32))
    return attn_out.astype(jnp.bfloat16)


def reference(hidden, positions, k_cache, v_cache, attn_norm, w_query, w_key, w_value, w_out, mlp_norm, w_gate, w_up, w_down):
    group = HEADS // KV_HEADS
    cos_tab, sin_tab = rope_tables(positions, HEAD)
    seq_ids = jnp.arange(SEQ)
    at_pos = (seq_ids[None, :] == positions[:, None])[:, :, None, None]
    visible = (seq_ids[None, :] <= positions[:, None])[:, None, None, :]

    def layer_step(state, layer_args):
        norm_attn, wq_layer, wk_layer, wv_layer, wo_layer, norm_mlp, wg_layer, wu_layer, wd_layer, k_layer, v_layer = layer_args
        normed = rms_norm(state, norm_attn)
        query = jnp.dot(normed, wq_layer, preferred_element_type=jnp.float32).astype(jnp.bfloat16)
        key_new = jnp.dot(normed, wk_layer, preferred_element_type=jnp.float32).astype(jnp.bfloat16)
        value_new = jnp.dot(normed, wv_layer, preferred_element_type=jnp.float32).astype(jnp.bfloat16)
        query = apply_rope(query.reshape(BATCH, HEADS, HEAD), cos_tab, sin_tab)
        key_new = apply_rope(key_new.reshape(BATCH, KV_HEADS, HEAD), cos_tab, sin_tab)
        value_new = value_new.reshape(BATCH, KV_HEADS, HEAD)
        k_layer = jnp.where(at_pos, key_new[:, None], k_layer)
        v_layer = jnp.where(at_pos, value_new[:, None], v_layer)
        attended = attend(query.reshape(BATCH, KV_HEADS, group, HEAD), k_layer, v_layer, visible)
        mixed = jnp.dot(attended.reshape(BATCH, HEADS * HEAD), wo_layer, preferred_element_type=jnp.float32)
        state = state + mixed.astype(jnp.bfloat16)
        normed = rms_norm(state, norm_mlp)
        gate_proj = jnp.dot(normed, wg_layer, preferred_element_type=jnp.float32).astype(jnp.bfloat16)
        up_proj = jnp.dot(normed, wu_layer, preferred_element_type=jnp.float32).astype(jnp.bfloat16)
        activated = (jax.nn.silu(gate_proj.astype(jnp.float32)) * up_proj.astype(jnp.float32)).astype(jnp.bfloat16)
        state = state + jnp.dot(activated, wd_layer, preferred_element_type=jnp.float32).astype(jnp.bfloat16)
        return state, (k_layer, v_layer)

    stacked = (attn_norm, w_query, w_key, w_value, w_out, mlp_norm, w_gate, w_up, w_down, k_cache, v_cache)
    final, (k_out, v_out) = lax.scan(layer_step, hidden, stacked)
    return final, k_out, v_out
```

```python
import math
import jax
import jax.numpy as jnp
from jax import lax
from jax.experimental import pallas as pl
from jax.experimental.pallas import tpu as pltpu
from jax.sharding import PartitionSpec as P

MESH = pl.DeviceIdType.MESH
F32 = jnp.float32
BF16 = jnp.bfloat16

ROWS = 128
WIDTH = 4096
CHUNK = 512
PIECES = WIDTH // CHUNK
HALF = ROWS // 2
QH = 8
HD = 128
SEQ = 64
KV2 = 2 * SEQ
FFL = 3584
NU = 10
N_Q, N_O, N_G, N_D = 3, 2, 14, 8
PER_LAYER = N_Q + N_O + N_G + N_D
LAYERS = 2
UNITS = LAYERS * PER_LAYER
GROUP = 16


def rope_tables(positions, head_dim):
    half_dim = head_dim // 2
    inv_freq = jnp.power(500000.0, -jnp.arange(half_dim, dtype=jnp.float32) * (2.0 / head_dim))
    wavelen = (2.0 * math.pi) / inv_freq
    smooth = (8192.0 / wavelen - 1.0) / 3.0
    blended = (1.0 - smooth) * inv_freq / 8.0 + smooth * inv_freq
    scaled = jnp.where(wavelen < 2048.0, inv_freq, jnp.where(wavelen > 8192.0, inv_freq / 8.0, blended))
    angles = positions.astype(jnp.float32)[:, None] * scaled[None, :]
    cos_tab, sin_tab = jnp.cos(angles), jnp.sin(angles)
    return jnp.stack([jnp.concatenate([cos_tab, cos_tab], -1), jnp.concatenate([-sin_tab, sin_tab], -1)])


def segments():
    segs = []
    for layer in range(LAYERS):
        base = layer * PER_LAYER
        segs.append(("q", layer, base, base + 2))
        segs.append(("kv", layer, base + 2, base + 3))
        segs.append(("o", layer, base + 3, base + 5))
        segs.append(("g", layer, base + 5, base + 19))
        segs.append(("d", layer, base + 19, base + 27))
    return segs


def layers_kernel(pos_ref, x_hbm, rope_hbm, an_hbm, mn_hbm, kc_hbm, vc_hbm, wq, wk, wv, wo, wg, wu, wd,
                  x_out, kn_out, vn_out,
                  wbuf, kbuf, vbuf, x_ref, h_ref, rope, anorm, mnorm, qbuf, obuf, ob16, knew, vnew, act,
                  part, ra, sb, rb, rc, rd,
                  wsem, csem, lsem, sa_s, sa_r, sb_s, sb_r, sc_s, sc_r, sd_s, sd_r):
    me = lax.axis_index("tp")
    core = lax.rem(me, 2)
    sibling = me + 1 - 2 * core
    across = lax.rem(me + 2, 4)
    mine = pl.ds(pl.multiple_of(core * HALF, HALF), HALF)
    other = pl.ds(pl.multiple_of((1 - core) * HALF, HALF), HALF)
    segs = segments()

    def copies(kind, layer, r, slot):
        col = pl.multiple_of(r * CHUNK, CHUNK) if kind != "g" else pl.multiple_of(r * 256, 256)
        if kind == "q":
            return [(wq.at[layer, :, pl.ds(col, CHUNK)], wbuf.at[slot])]
        if kind == "kv":
            return [(wk.at[layer], wbuf.at[slot, :, pl.ds(0, 256)]), (wv.at[layer], wbuf.at[slot, :, pl.ds(256, 256)])]
        if kind == "o":
            return [(wo.at[layer, :, pl.ds(pl.multiple_of((r * 4 + s) * CHUNK, CHUNK), CHUNK)],
                     wbuf.at[slot, pl.ds(s * 1024, 1024), :]) for s in range(4)]
        if kind == "g":
            return [(wg.at[layer, :, pl.ds(col, 256)], wbuf.at[slot, :, pl.ds(0, 256)]),
                    (wu.at[layer, :, pl.ds(col, 256)], wbuf.at[slot, :, pl.ds(256, 256)])]
        return [(wd.at[layer, :, pl.ds(col, CHUNK)], wbuf.at[slot, pl.ds(0, FFL), :])]

    def issue(t, lo, hi):
        for kind, layer, s, e in segs:
            if e <= lo or s >= hi:
                continue

            def go(kind=kind, layer=layer, s=s):
                slot = lax.rem(t, NU)
                for src, dst in copies(kind, layer, t - s, slot):
                    pltpu.make_async_copy(src, dst, wsem.at[slot]).start()

            if s <= lo and hi <= e:
                go()
            else:
                pl.when((t >= s) & (t < e))(go)

    def wait_unit(slot, down=False):
        if down:
            src, dst = wd.at[0, :, pl.ds(0, CHUNK)], wbuf.at[slot, pl.ds(0, FFL), :]
        else:
            src, dst = wq.at[0, :, pl.ds(0, CHUNK)], wbuf.at[slot]
        pltpu.make_async_copy(src, dst, wsem.at[slot]).wait()

    def cache_copies(layer):
        return [pltpu.make_async_copy(kc_hbm.at[layer], kbuf, csem.at[0]),
                pltpu.make_async_copy(vc_hbm.at[layer], vbuf, csem.at[1])]

    small = [pltpu.make_async_copy(x_hbm, x_ref, lsem.at[0]), pltpu.make_async_copy(an_hbm, anorm, lsem.at[1]),
             pltpu.make_async_copy(rope_hbm, rope, lsem.at[2]), pltpu.make_async_copy(mn_hbm, mnorm, lsem.at[3])]
    for c in small:
        c.start()
    for t in range(3):
        issue(jnp.int32(t), t, t + 1)
    for c in cache_copies(0):
        c.start()
    for t in range(3, NU):
        issue(jnp.int32(t), t, t + 1)

    barrier = pltpu.get_barrier_semaphore()
    for dev in (sibling, across):
        pl.semaphore_signal(barrier, inc=1, device_id={"tp": dev}, device_id_type=MESH)
    pl.semaphore_wait(barrier, 2)
    small[0].wait()
    small[1].wait()

    def lanes(j, n):
        return pl.ds(pl.multiple_of(j * n, n), n)

    def sum_sq(v):
        sq = v * v
        acc = sq[:, 0:128]
        for k in range(1, v.shape[1] // 128):
            acc = acc + sq[:, k * 128:(k + 1) * 128]
        return acc

    def normalize(acc, norm, layer):
        mean_sq = jnp.sum(acc, axis=-1, keepdims=True) * (1.0 / WIDTH)
        scale = lax.rsqrt(mean_sq + 1e-5)

        def body(j, carry):
            w = norm[:, lanes(j, CHUNK)].astype(F32)[layer:layer + 1, :]
            xv = x_ref[:, lanes(j, CHUNK)].astype(F32)
            h_ref[:, lanes(j, CHUNK)] = (xv * scale * w).astype(BF16)
            return carry

        lax.fori_loop(0, PIECES, body, 0)

    def remote(src, dst, send, recv, dev):
        return pltpu.make_async_remote_copy(src_ref=src, dst_ref=dst, send_sem=send, recv_sem=recv,
                                            device_id={"tp": dev}, device_id_type=MESH)

    def copy_a(p, j):
        return remote(part.at[j, other, :], ra.at[p, j], sa_s.at[j], sa_r.at[p, j], sibling)

    def copy_b(p, j):
        return remote(sb.at[j], rb.at[p, j], sb_s.at[j], sb_r.at[p, j], across)

    def copy_c(p, j):
        return remote(sb.at[j], rc.at[p, j], sc_s.at[j], sc_r.at[p, j], sibling)

    def copy_d(p, j):
        return remote(rb.at[p, j], rd.at[p, j], sd_s.at[j], sd_r.at[p, j], sibling)

    def stage_a(p, j):
        copy_a(p, j).wait_recv()
        total = part[j, mine, :].astype(F32) + ra[p, j].astype(F32)
        sb[j] = total.astype(BF16)
        copy_b(p, j).start()
        copy_c(p, j).start()

    def finish(p, lag):
        for j in range(PIECES - lag, PIECES):
            stage_a(p, j)

        def add(j):
            cols = lanes(j, CHUNK)
            near = (sb[j].astype(F32) + rb[p, j].astype(F32)).astype(BF16).astype(F32)
            new = (x_ref[mine, cols].astype(F32) + near).astype(BF16)
            x_ref[mine, cols] = new
            copy_c(p, j).wait_recv()
            copy_d(p, j).wait_recv()
            far = (rc[p, j].astype(F32) + rd[p, j].astype(F32)).astype(BF16).astype(F32)
            new = (x_ref[other, cols].astype(F32) + far).astype(BF16)
            x_ref[other, cols] = new
            copy_a(p, j).wait_send()
            copy_b(p, j).wait_send()
            copy_c(p, j).wait_send()
            copy_d(p, j).wait_send()
            return sum_sq(x_ref[:, cols].astype(F32))

        def forward(j):
            copy_b(p, j).wait_recv()
            copy_d(p, j).start()

        forward(0)

        def body(j, acc):
            forward(j)
            return acc + add(j - 1)

        acc = lax.fori_loop(1, PIECES, body, jnp.zeros((ROWS, 128), F32))
        return acc + add(PIECES - 1)

    row_id = lax.broadcasted_iota(jnp.int32, (16, 256), 0)
    col_id = lax.broadcasted_iota(jnp.int32, (16, 256), 1)
    fits = ((row_id // 8) == (col_id // KV2)) & (((row_id % 8) // 4) == (col_id % 2))
    limit = jnp.where(fits, (col_id % KV2) // 2, 1 << 20)
    first_req = col_id < KV2
    pair_row = (lax.broadcasted_iota(jnp.int32, (KV2, HD), 0) // 2).astype(F32).astype(BF16)
    odd = (lax.broadcasted_iota(jnp.int32, (16, HD), 0) % 2) == 1

    def with_new(buf, new, b, pos):
        old = buf[pl.ds(pl.multiple_of(b * KV2, KV2), KV2), :]
        tile = jnp.where(odd, new[1:2, :], new[0:1, :]).astype(BF16)
        fresh = jnp.concatenate([tile] * (KV2 // 16), axis=0)
        here = pair_row == jnp.full((KV2, HD), pos.astype(F32), F32).astype(BF16)
        return jnp.where(here, fresh, old)

    def attention():
        def body(g, carry):
            kn = knew[pl.ds(pl.multiple_of(g * 2 * GROUP, 2 * GROUP), 2 * GROUP), :]
            vn = vnew[pl.ds(pl.multiple_of(g * 2 * GROUP, 2 * GROUP), 2 * GROUP), :]
            for pr in range(GROUP // 2):
                b0 = g * GROUP + 2 * pr
                p0, p1 = pos_ref[b0], pos_ref[b0 + 1]
                at = 4 * pr
                kk = jnp.concatenate([with_new(kbuf, kn[at:at + 2], b0, p0), with_new(kbuf, kn[at + 2:at + 4], b0 + 1, p1)], axis=0)
                vv = jnp.concatenate([with_new(vbuf, vn[at:at + 2], b0, p0), with_new(vbuf, vn[at + 2:at + 4], b0 + 1, p1)], axis=0)
                q2 = qbuf[pl.ds(pl.multiple_of(b0 * QH, 16), 16), :].astype(BF16)
                sc = lax.dot_general(q2, kk, (((1,), (1,)), ((), ())), preferred_element_type=F32) * (HD ** -0.5)
                sc = jnp.where(limit <= jnp.where(first_req, p0, p1), sc, -jnp.inf)
                ex = jnp.exp(sc - jnp.max(sc, axis=-1, keepdims=True))
                prob = (ex * (1.0 / jnp.sum(ex, axis=-1, keepdims=True))).astype(BF16)
                o = jnp.dot(prob, vv, preferred_element_type=F32)
                obuf[pl.ds(pl.multiple_of(b0 * QH, 16), 16), :] = o
            return carry

        lax.fori_loop(0, ROWS // GROUP, body, 0)
        for j in range(QH):
            ob16[:, j * HD:(j + 1) * HD] = obuf[pl.ds(j, ROWS, stride=QH), :].astype(BF16)

    def first_sq(j, acc):
        return acc + sum_sq(x_ref[:, lanes(j, CHUNK)].astype(F32))

    acc = lax.fori_loop(0, PIECES, first_sq, jnp.zeros((ROWS, 128), F32))
    for layer in range(LAYERS):
        base = layer * PER_LAYER
        normalize(acc, anorm, layer)
        if layer == 0:
            small[2].wait()
            small[3].wait()

        for i in range(N_Q):
            t = base + i
            slot = t % NU
            wait_unit(slot)
            res = jnp.dot(h_ref[...], wbuf[slot], preferred_element_type=F32).astype(BF16).astype(F32)
            if t + NU < UNITS:
                issue(jnp.int32(t + NU), t + NU, t + NU + 1)
            for hh in range(CHUNK // HD):
                v = res[:, hh * HD:(hh + 1) * HD]
                if i < 2 or hh < 2:
                    v = v * rope[0] + pltpu.roll(v, HD // 2, 1) * rope[1]
                    v = v.astype(BF16).astype(F32)
                if i < 2:
                    qbuf[pl.ds(i * 4 + hh, ROWS, stride=QH), :] = v
                elif hh < 2:
                    knew[pl.ds(hh, ROWS, stride=2), :] = v
                else:
                    vnew[pl.ds(hh - 2, ROWS, stride=2), :] = v
        kn_out[layer] = knew[...].astype(BF16)
        vn_out[layer] = vnew[...].astype(BF16)

        for c in cache_copies(layer):
            c.wait()
        attention()
        if layer + 1 < LAYERS:
            for c in cache_copies(layer + 1):
                c.start()

        p = 0
        lag_o = 4
        for u in range(N_O):
            t = base + N_Q + u
            slot = t % NU
            wait_unit(slot)

            def out_piece(s, carry, u=u, slot=slot):
                j = u * 4 + s
                w = wbuf[slot, pl.ds(pl.multiple_of(s * 1024, 1024), 1024), :]
                part[j] = jnp.dot(ob16[...], w, preferred_element_type=F32).astype(BF16)
                copy_a(p, j).start()

                @pl.when(j >= lag_o)
                def _():
                    stage_a(p, j - lag_o)

                return carry

            lax.fori_loop(0, 4, out_piece, 0)
            if t + NU < UNITS:
                issue(jnp.int32(t + NU), t + NU, t + NU + 1)
        acc = finish(p, lag_o)
        normalize(acc, mnorm, layer)

        def gate_up(i, carry):
            t = base + N_Q + N_O + i
            slot = lax.rem(t, NU)
            wait_unit(slot)
            res = jnp.dot(h_ref[...], wbuf[slot], preferred_element_type=F32).astype(BF16).astype(F32)
            lo = base + N_Q + N_O + NU

            if lo + N_G <= UNITS:
                issue(t + NU, lo, lo + N_G)
            else:
                issue(t + NU, lo, UNITS)
            gate, up = res[:, :256], res[:, 256:]
            act[:, lanes(i, 256)] = (gate * (1.0 / (1.0 + jnp.exp(-gate))) * up).astype(BF16)
            return carry

        lax.fori_loop(0, N_G, gate_up, 0)

        p = 1
        lag_d = 2

        def down_piece(j, carry):
            t = base + N_Q + N_O + N_G + j
            slot = lax.rem(t, NU)
            wait_unit(slot, down=True)
            part[j] = jnp.dot(act[...], wbuf[slot, pl.ds(0, FFL), :], preferred_element_type=F32).astype(BF16)
            copy_a(p, j).start()
            lo = base + N_Q + N_O + N_G + NU
            if lo < UNITS:
                issue(t + NU, lo, min(lo + N_D, UNITS))

            @pl.when(j >= lag_d)
            def _():
                stage_a(p, j - lag_d)

            return carry

        lax.fori_loop(0, N_D, down_piece, 0)
        acc = finish(p, lag_d)

    x_out[...] = x_ref[...]


def run_layers(positions, hidden, rope, attn_norm, mlp_norm, kc, vc, wq, wk, wv, wo, wg, wu, wd):
    any_spec = pl.BlockSpec(memory_space=pl.ANY)
    vmem = pl.BlockSpec(memory_space=pltpu.VMEM)
    dma = pltpu.SemaphoreType.DMA
    piece = (PIECES, HALF, CHUNK)
    return pl.pallas_call(
        layers_kernel,
        name="layers",
        out_shape=(jax.ShapeDtypeStruct((ROWS, WIDTH), BF16),
                   jax.ShapeDtypeStruct((LAYERS, 2 * ROWS, HD), BF16),
                   jax.ShapeDtypeStruct((LAYERS, 2 * ROWS, HD), BF16)),
        in_specs=[pl.BlockSpec(memory_space=pltpu.SMEM)] + [any_spec] * 13,
        out_specs=(vmem, vmem, vmem),
        scratch_shapes=[
            pltpu.VMEM((NU, WIDTH, CHUNK), BF16),
            pltpu.VMEM((ROWS * KV2, HD), BF16),
            pltpu.VMEM((ROWS * KV2, HD), BF16),
            pltpu.VMEM((ROWS, WIDTH), BF16),
            pltpu.VMEM((ROWS, WIDTH), BF16),
            pltpu.VMEM((2, ROWS, HD), F32),
            pltpu.VMEM((LAYERS, WIDTH), BF16),
            pltpu.VMEM((LAYERS, WIDTH), BF16),
            pltpu.VMEM((ROWS * QH, HD), F32),
            pltpu.VMEM((ROWS * QH, HD), F32),
            pltpu.VMEM((ROWS, QH * HD), BF16),
            pltpu.VMEM((2 * ROWS, HD), F32),
            pltpu.VMEM((2 * ROWS, HD), F32),
            pltpu.VMEM((ROWS, FFL), BF16),
            pltpu.VMEM((PIECES, ROWS, CHUNK), BF16),
            pltpu.VMEM((2,) + piece, BF16),
            pltpu.VMEM(piece, BF16),
            pltpu.VMEM((2,) + piece, BF16),
            pltpu.VMEM((2,) + piece, BF16),
            pltpu.VMEM((2,) + piece, BF16),
            dma((NU,)), dma((2,)), dma((4,)),
            dma((PIECES,)), dma((2, PIECES)), dma((PIECES,)), dma((2, PIECES)),
            dma((PIECES,)), dma((2, PIECES)), dma((PIECES,)), dma((2, PIECES)),
        ],
        compiler_params=pltpu.CompilerParams(collective_id=0, has_side_effects=True, vmem_limit_bytes=67043328),
    )(positions, hidden, rope, attn_norm, mlp_norm, kc, vc, wq, wk, wv, wo, wg, wu, wd)


BLOCK = 32
CACHE_BLOCKS = LAYERS * ROWS // BLOCK


def cache_kernel(pos_ref, kc, vc, kn, vn, ko, vo, buf, isem, osem):
    where = [(which, layer, b) for layer in range(LAYERS) for b in range(0, ROWS, BLOCK) for which in range(2)]
    ins, outs = [], []
    for n, (which, layer, b) in enumerate(where):
        ins.append(pltpu.make_async_copy((kc, vc)[which].at[layer, pl.ds(b, BLOCK)], buf.at[n], isem.at[n]))
        outs.append(pltpu.make_async_copy(buf.at[n], (ko, vo)[which].at[layer, pl.ds(b, BLOCK)], osem.at[n]))
    for c in ins:
        c.start()
    for n, (which, layer, b) in enumerate(where):
        ins[n].wait()
        new = (kn, vn)[which]

        def row(i, carry, n=n, layer=layer, b=b, new=new):
            buf[n, i, pos_ref[b + i]] = new[layer, b + i]
            return carry

        lax.fori_loop(0, BLOCK, row, 0, unroll=8)
        outs[n].start()
    for c in outs:
        c.wait()


def write_cache(positions, k_cache, v_cache, k_new, v_new):
    any_spec = pl.BlockSpec(memory_space=pl.ANY)
    vmem = pl.BlockSpec(memory_space=pltpu.VMEM)
    return pl.pallas_call(
        cache_kernel,
        name="cache",
        out_shape=(jax.ShapeDtypeStruct(k_cache.shape, BF16), jax.ShapeDtypeStruct(v_cache.shape, BF16)),
        in_specs=[pl.BlockSpec(memory_space=pltpu.SMEM), any_spec, any_spec, vmem, vmem],
        out_specs=(any_spec, any_spec),
        scratch_shapes=[pltpu.VMEM((2 * CACHE_BLOCKS, BLOCK, SEQ, 2, HD), BF16),
                        pltpu.SemaphoreType.DMA((2 * CACHE_BLOCKS,)), pltpu.SemaphoreType.DMA((2 * CACHE_BLOCKS,))],
        compiler_params=pltpu.CompilerParams(vmem_limit_bytes=67043328),
    )(positions, k_cache, v_cache, k_new, v_new)


def solution(mesh):
    row_spec = P('dp', None)
    pos_spec = P('dp')
    cache_spec = P(None, 'dp', None, 'tp', None)
    norm_spec = P(None, None)
    col_spec = P(None, None, 'tp')
    split_rows = P(None, 'tp', None)

    def local_step(hidden, positions, k_cache, v_cache, attn_norm, w_query, w_key, w_value, w_out, mlp_norm, w_gate, w_up, w_down):
        rope = rope_tables(positions, HD)
        flat = (LAYERS, ROWS * KV2, HD)
        x, k_new, v_new = run_layers(positions, hidden, rope, attn_norm, mlp_norm, k_cache.reshape(flat), v_cache.reshape(flat),
                                     w_query, w_key, w_value, w_out, w_gate, w_up, w_down)
        pair = (LAYERS, ROWS, 2, HD)
        k_out, v_out = write_cache(positions, k_cache, v_cache, k_new.reshape(pair), v_new.reshape(pair))
        return x, k_out, v_out

    return jax.shard_map(local_step, mesh=mesh, in_specs=(row_spec, pos_spec, cache_spec, cache_spec, norm_spec, col_spec, col_spec, col_spec, split_rows, norm_spec, col_spec, col_spec, split_rows), out_specs=(row_spec, cache_spec, cache_spec), check_vma=False)
```
